32 devices in a mesh: outer: 4 (over z), mid: 2 (over y), inner: 4 (over x, core).
Axes of the slice: x: 2, y: 2, z: 4, core: 2. Of those that a mesh axis runs over, the one named last changes fastest.
Arguments:
- x: bfloat16 [4096, 2048], P(('outer', 'mid', 'inner'))
- ids: int32 [4096, 6], P(('outer', 'mid', 'inner'))
- gates: float32 [4096, 6], P(('outer', 'mid', 'inner'))
- w1: bfloat16 [64, 2048, 1408], P(('outer', 'mid', 'inner'))
- w3: bfloat16 [64, 2048, 1408], P(('outer', 'mid', 'inner'))
- w2: bfloat16 [64, 1408, 2048], P(('outer', 'mid', 'inner'))
- ws1: bfloat16 [2048, 2816], replicated
- ws3: bfloat16 [2048, 2816], replicated
- ws2: bfloat16 [2816, 2048], replicated
Outputs:
- output: bfloat16 [4096, 2048], P(('outer', 'mid', 'inner'))
All inputs are finite; a program needn't handle non-finite values.
Results may differ from the reference program's by a relative error of at most 0.00633531.
Values are sent between devices in bfloat16 or wider.
A program may use at most 1 GiB of HBM per device.

```python
import jax
import jax.numpy as jnp
from jax import lax

T = 128
DEV = 32
H = 2048
E = 64
F = 1408
FS = 2816
TOP = 6
GROUPS = 1
TOPG = 1
CAP = 48

TOKENS = DEV * T
EPD = E // DEV
EPG = E // GROUPS


def route(noise_e, noise_g):
    need = (TOP + TOPG - 1) // TOPG
    devs = jnp.arange(DEV)
    grp = jnp.arange(GROUPS)

    def step(cnt, inp):
        ne, ng = inp
        ex_ok = jnp.repeat(cnt < CAP, EPD)
        avail = jnp.sum(ex_ok.reshape(GROUPS, EPG).astype(jnp.int32), axis=1)
        gsel = lax.top_k(jnp.where(avail >= need, ng, jnp.int32(-1)), TOPG)[1]
        gmask = jnp.any(gsel[:, None] == grp[None, :], axis=0)
        esc = jnp.where(ex_ok & jnp.repeat(gmask, EPG), ne, jnp.int32(-1))
        sel = lax.top_k(esc, TOP)[1]
        hitd = jnp.any((sel // EPD)[:, None] == devs[None, :], axis=0)
        return cnt + hitd.astype(jnp.int32), sel.astype(jnp.int32)

    def one_dev(ne, ng):
        return lax.scan(step, jnp.zeros((DEV,), jnp.int32), (ne, ng))[1]

    return jax.vmap(one_dev)(noise_e, noise_g).reshape(TOKENS, TOP)


def draw_experts(k, n_in, n_out):
    def one(kk):
        return (jax.random.normal(kk, (n_in, n_out), jnp.float32) * n_in ** -0.5).astype(jnp.bfloat16)
    return lax.map(one, jax.random.split(k, E))


def setup_inputs(seed: int = 0) -> dict:
    ks = jax.random.split(jax.random.key(seed), 10)
    kd = jax.random.split(jax.random.fold_in(jax.random.key(seed), 7), 3)
    x = jax.random.normal(ks[0], (TOKENS, H), jnp.float32).astype(jnp.bfloat16)
    hot = (jax.random.uniform(kd[0], (E,), jnp.float32) < 0.12).astype(jnp.int32)
    tilt = (jnp.arange(E) // EPD).astype(jnp.int32)
    bias_e = 629146 * hot + 52429 * tilt
    bias_g = 524288 * (jnp.arange(GROUPS) < 2).astype(jnp.int32)
    base_e = (jax.random.bits(kd[1], (DEV, T, E), jnp.uint32) >> 12).astype(jnp.int32)
    base_g = (jax.random.bits(kd[2], (DEV, T, GROUPS), jnp.uint32) >> 12).astype(jnp.int32)
    noise_e = (base_e + bias_e) * E + (E - 1 - jnp.arange(E, dtype=jnp.int32))
    noise_g = (base_g + bias_g) * GROUPS + (GROUPS - 1 - jnp.arange(GROUPS, dtype=jnp.int32))
    ids = route(noise_e, noise_g)
    u = jax.random.uniform(ks[3], (TOKENS, TOP), jnp.float32, 0.5, 1.5)
    gates = 2.5 * u / jnp.sum(u, axis=1, keepdims=True)
    w1 = draw_experts(ks[4], H, F)
    w3 = draw_experts(ks[5], H, F)
    w2 = draw_experts(ks[6], F, H)
    ws1 = (jax.random.normal(ks[7], (H, FS), jnp.float32) * H ** -0.5).astype(jnp.bfloat16)
    ws3 = (jax.random.normal(ks[8], (H, FS), jnp.float32) * H ** -0.5).astype(jnp.bfloat16)
    ws2 = (jax.random.normal(ks[9], (FS, H), jnp.float32) * FS ** -0.5).astype(jnp.bfloat16)
    return {"x": x, "ids": ids, "gates": gates, "w1": w1, "w3": w3, "w2": w2, "ws1": ws1, "ws3": ws3, "ws2": ws2}


def routed_sum(x, ids, gates, w1, w3, w2):
    blk = 16
    n = x.shape[0]
    flat = ids.reshape(-1)
    order = jnp.argsort(flat)
    counts = jnp.zeros((E,), jnp.int32).at[flat].add(1)
    starts = jnp.cumsum(counts) - counts
    ntile = (counts + blk - 1) // blk
    tend = jnp.cumsum(ntile)
    tstart = tend - ntile
    gflat = gates.reshape(-1)
    lanes = jnp.arange(blk)

    def body(i, acc):
        e = jnp.sum((tend <= i).astype(jnp.int32))
        r = (i - tstart[e]) * blk + lanes
        ok = r < counts[e]
        a = order[jnp.minimum(starts[e] + r, n * TOP - 1)]
        src = a // TOP
        g = jnp.where(ok, gflat[a], 0.0)
        xa = x[src]
        a1 = jnp.dot(xa, w1[e], preferred_element_type=jnp.float32)
        a3 = jnp.dot(xa, w3[e], preferred_element_type=jnp.float32)
        h = (jax.nn.silu(a1) * a3).astype(jnp.bfloat16)
        o = jnp.dot(h, w2[e], preferred_element_type=jnp.float32)
        return acc.at[src].add(g[:, None] * o)

    return lax.fori_loop(0, tend[-1], body, jnp.zeros((n, x.shape[1]), jnp.float32))


def reference(x, ids, gates, w1, w3, w2, ws1, ws3, ws2):
    moe = routed_sum(x, ids, gates, w1, w3, w2)
    s1 = jnp.dot(x, ws1, preferred_element_type=jnp.float32)
    s3 = jnp.dot(x, ws3, preferred_element_type=jnp.float32)
    hs = (jax.nn.silu(s1) * s3).astype(jnp.bfloat16)
    sh = jnp.dot(hs, ws2, preferred_element_type=jnp.float32)
    return (x.astype(jnp.float32) + sh + moe).astype(jnp.bfloat16)
```

```python
import functools

import jax
import jax.numpy as jnp
from jax import lax
from jax.experimental import pallas as pl
from jax.experimental.pallas import tpu as pltpu
from jax.sharding import PartitionSpec as P

CAP = 48
TN = 256
MESH = pl.DeviceIdType.MESH
F32 = jnp.float32
BF16 = jnp.bfloat16


def cut(text, n):
    return [text[i:i + n] for i in range(0, len(text), n)]


def rel(name):
    return int(name[1]) * 4 + "CXYD".index(name[0])


class Place:
    def __init__(self, axes):
        o, m, i = axes
        self.axes = axes
        self.z = lax.axis_index(o)
        self.y = lax.axis_index(m)
        inner = lax.axis_index(i)
        self.x = inner // 2
        self.c = inner % 2
        self.me = self.z * 8 + self.y * 4 + inner
        self.mate = self.me + 1 - 2 * self.c
        self.mid = jnp.logical_and(self.z >= 1, self.z <= 2)
        self.z1 = self.z + 1 - 2 * (self.z % 2)
        self.z3 = 3 - self.z

    def dev(self, z, y, x, c):
        o, m, i = self.axes
        return {o: z, m: y, i: x * 2 + c}

    def target(self, name):
        z, y, x, c = self.z, self.y, self.x, self.c
        return {
            "X": self.dev(z, y, 1 - x, c),
            "Y": self.dev(z, 1 - y, x, c),
            "P": self.dev(z, y, x, 1 - c),
            "Z1": self.dev(self.z1, y, x, c),
            "Z3": self.dev(self.z3, y, x, c),
        }[name]


FLIP = {"X": 1, "Y": 2, "Z1": 4, "Z3": 12, "P": 0}


def barrier(pos):
    sem = pltpu.get_barrier_semaphore()
    for t in ("X", "Y", "P", "Z1"):
        pl.semaphore_signal(sem, inc=1, device_id=pos.target(t), device_id_type=MESH)

    @pl.when(pos.mid)
    def _():
        pl.semaphore_signal(sem, inc=1, device_id=pos.target("Z3"), device_id_type=MESH)
        pl.semaphore_wait(sem, 5)

    @pl.when(jnp.logical_not(pos.mid))
    def _():
        pl.semaphore_wait(sem, 4)


def slots(meta, dev, tri):
    ids = meta[0:8, :]
    gat = meta[8:16, :]
    e0 = (2 * dev).astype(F32)
    m0 = ids == e0
    m1 = ids == e0 + 1.0
    g0 = jnp.sum(jnp.where(m0, gat, 0.0), axis=0, keepdims=True)
    g1 = jnp.sum(jnp.where(m1, gat, 0.0), axis=0, keepdims=True)
    hit = jnp.sum(jnp.where(m0, 1.0, 0.0) + jnp.where(m1, 1.0, 0.0), axis=0, keepdims=True) > 0.5
    hitf = jnp.broadcast_to(jnp.where(hit, 1.0, 0.0), (8, ids.shape[1])).astype(BF16)
    pos = jnp.dot(hitf, tri, preferred_element_type=F32)[0:1, :]
    row = lax.broadcasted_iota(jnp.int32, (CAP, ids.shape[1]), 0).astype(F32)
    oh = jnp.where(jnp.logical_and(row == pos, jnp.where(hit, 1.0, 0.0) > 0.5), 1.0, 0.0)
    return oh, g0, g1


def strict_upper(t):
    a = lax.broadcasted_iota(jnp.int32, (t, t), 0)
    b = lax.broadcasted_iota(jnp.int32, (t, t), 1)
    return jnp.where(a < b, 1.0, 0.0).astype(BF16)


GROUPS = [cut(g, 2) for g in ("C0X0Y0C1", "X1Y1C2C3", "X2Y2D0D1", "X3Y3D2D3")]
EVENTS = {
    1: "C1XC1YC13C31Y0XY0PX0PC1P",
    2: "C2XC2YC21X1YX1PY1PC2P",
    3: "C3XC3YY2XY2PD0PC3P",
    4: "X2PD1P",
    5: "X3YX3PY3P",
    6: "D2PD3P",
}


def expert_kernel(axes, x_ref, m_ref, w1_ref, w3_ref, w2_ref, os_ref, op_ref, mo_ref,
                  xall, mall, w13, w2v, xg, hbuf, gbuf, obuf,
                  xs, xr, ms, mr, ls, ws, w2s, osem, pss, prs):
    pos = Place(axes)
    t, hdim = x_ref.shape
    nf = w1_ref.shape[2] // 128
    nn = hdim // TN
    barrier(pos)
    sends = []

    def send(b, name, own=False):
        dst = rel(b) ^ FLIP[name]
        dc = int(name == "P")
        n = len(sends)

        def make():
            out = []
            for ref, full, ss, rs in ((m_ref, mall, ms, mr), (x_ref, xall, xs, xr)):
                src = ref if own else full.at[0, rel(b)]
                out.append(pltpu.make_async_remote_copy(src, full.at[dc, dst], ss.at[n], rs.at[dc, dst],
                                                        device_id=pos.target(name), device_id_type=MESH))
            return out
        for c in make():
            c.start()
        sends.append(make)

    def arrived(b, dc):
        for ref, full, ss, rs in ((m_ref, mall, ms, mr), (x_ref, xall, xs, xr)):
            pltpu.make_async_remote_copy(ref, full.at[dc, rel(b)], ss.at[0], rs.at[dc, rel(b)],
                                         device_id=pos.target("X"), device_id_type=MESH).wait_recv()

    mid_sends = []

    def mid_send(b, name, own=False):
        pl.when(pos.mid)(lambda: send(b, name, own))
        mid_sends.append(len(sends) - 1)

    for name in ("X", "Y", "Z1"):
        send("C0", name, True)
    mid_send("C0", "Z3", True)
    send("C0", "P", True)
    lx = pltpu.make_async_copy(x_ref, xall.at[0, 0], ls.at[0])
    lm = pltpu.make_async_copy(m_ref, mall.at[0, 0], ls.at[1])
    lx.start()
    lm.start()

    def w13_copy(i, half):
        e, j = i // nf, i % nf
        src = w1_ref if half == 0 else w3_ref
        return pltpu.make_async_copy(src.at[e, :, pl.ds(pl.multiple_of(j * 128, 128), 128)],
                                     w13.at[i, :, pl.ds(half * 128, 128)], ws.at[half, i])

    def w2_copy(i):
        e, n = i // nn, i % nn
        return pltpu.make_async_copy(w2_ref.at[e, :, pl.ds(pl.multiple_of(n * TN, TN), TN)], w2v.at[i], w2s.at[i])

    def start_w13(i, _):
        w13_copy(i, 0).start()
        w13_copy(i, 1).start()
        return 0

    def start_w2(i, _):
        w2_copy(i).start()
        return 0

    lax.fori_loop(0, 2 * nf, start_w13, 0)
    lax.fori_loop(0, 2 * nn, start_w2, 0)

    seen = set()

    def event(n):
        for step in cut(EVENTS[n], 3):
            b, to = step[:2], step[2]
            if b == "C3" and n == 1:
                pl.when(pos.mid)(lambda: arrived(b, 0))
            elif b == "C3" and b not in seen:
                pl.when(jnp.logical_not(pos.mid))(lambda: arrived(b, 0))
                seen.add(b)
            elif b not in seen:
                arrived(b, 0)
                seen.add(b)
            if to in "13":
                mid_send(b, "Z" + to)
            else:
                send(b, to)

    tri = strict_upper(t)
    outs = {}

    def gather_rows(group):
        for i, b in enumerate(group):
            for dc in range(2):
                if dc == 1:
                    arrived(b, 1)
                s = rel(b)
                oh, g0, g1 = slots(mall[dc, s], pos.me, tri)
                r0 = (dc * 4 + i) * CAP
                xg[r0:r0 + CAP, :] = jnp.dot(oh.astype(BF16), xall[dc, s], preferred_element_type=F32).astype(BF16)
                gbuf[0, r0:r0 + CAP, :] = jnp.broadcast_to(jnp.sum(oh * g0, axis=1, keepdims=True), (CAP, 128))
                gbuf[1, r0:r0 + CAP, :] = jnp.broadcast_to(jnp.sum(oh * g1, axis=1, keepdims=True), (CAP, 128))

    def up(e, first):
        def body(j, _):
            i = e * nf + j
            if first:
                w13_copy(i, 0).wait()
                w13_copy(i, 1).wait()
            a = jnp.dot(xg[...], w13[i], preferred_element_type=F32)
            h = (jax.nn.silu(a[:, :128]) * a[:, 128:]).astype(BF16)
            hbuf[e, :, pl.ds(pl.multiple_of(j * 128, 128), 128)] = h
            return 0
        lax.fori_loop(0, nf, body, 0)

    def down(g, first):
        def body(n, _):
            if first:
                w2_copy(n).wait()
                w2_copy(nn + n).wait()
            o0 = jnp.dot(hbuf[0], w2v[n], preferred_element_type=F32)
            o1 = jnp.dot(hbuf[1], w2v[nn + n], preferred_element_type=F32)
            o = gbuf[0, :, 0:1] * o0 + gbuf[1, :, 0:1] * o1
            obuf[g % 2, :, pl.ds(pl.multiple_of(n * TN, TN), TN)] = o.astype(BF16)
            return 0
        lax.fori_loop(0, nn, body, 0)

    def put(g):
        outs[g] = []
        for i, b in enumerate(GROUPS[g]):
            s = rel(b)
            q = 4 * g + i
            a = pltpu.make_async_copy(obuf.at[g % 2, pl.ds(i * CAP, CAP), :], os_ref.at[s], osem.at[q])
            r = pltpu.make_async_remote_copy(obuf.at[g % 2, pl.ds((4 + i) * CAP, CAP), :], op_ref.at[s], pss.at[q],
                                             prs.at[q], device_id=pos.target("P"), device_id_type=MESH)
            r.start()
            a.start()
            outs[g].append((a, r))

    def put_done(g):
        for a, r in outs[g]:
            a.wait()
            r.wait_send()

    event(1)
    lx.wait()
    lm.wait()
    gather_rows(GROUPS[0])
    up(0, True)
    up(1, True)
    event(2)
    down(0, True)
    put(0)
    event(3)
    gather_rows(GROUPS[1])
    up(0, False)
    up(1, False)
    event(4)
    down(1, False)
    put(1)
    gather_rows(GROUPS[2])
    up(0, False)
    event(5)
    up(1, False)
    put_done(0)
    down(2, False)
    put(2)
    event(6)
    gather_rows(GROUPS[3])
    up(0, False)
    up(1, False)
    put_done(1)
    down(3, False)
    put(3)
    mo_ref[...] = mall[0]
    for n, make in enumerate(sends):
        def done(make=make):
            for c in make():
                c.wait_send()
        if n in mid_sends:
            pl.when(pos.mid)(done)
        else:
            done()
    put_done(2)
    put_done(3)
    for g in range(4):
        for a, r in outs[g]:
            r.wait_recv()


SLOTS = cut("dX3dX1dY2dY0cX0cX1cX2cX3cY0cY1cY2cY3az0az2az3bz0bz1", 3)
HOPS = {"1": "bz1az0az0", "2": "az2bz1az3", "3": "az3bz0az2"}


def combine_kernel(axes, os_ref, op_ref, m_ref, x_ref, v1_ref, v3_ref, v2_ref, y_ref,
                   ov, sbuf, rbuf, w13, w2v, hs, sh, xv,
                   osem, ssem, rsem, ws, w2s, ls):
    pos = Place(axes)
    t, hdim = x_ref.shape
    nf = v1_ref.shape[1] // 128
    nn = hdim // TN
    order = [rel(b) for b in cut("D3D2D1D0X3Y3X2Y2X1Y1X0Y0C3C2C1C0", 2)]

    def o_copy(s, h):
        src = os_ref if h == 0 else op_ref
        return pltpu.make_async_copy(src.at[s], ov.at[s, pl.ds(h * CAP, CAP), :], osem.at[h, s])

    for s in order:
        o_copy(s, 0).start()
        o_copy(s, 1).start()
    lx = pltpu.make_async_copy(x_ref, xv, ls.at[0])
    lx.start()

    def w13_copy(i, half):
        src = v1_ref if half == 0 else v3_ref
        return pltpu.make_async_copy(src.at[:, pl.ds(pl.multiple_of(i * 128, 128), 128)],
                                     w13.at[i, :, pl.ds(half * 128, 128)], ws.at[half, i])

    def w2_copy(n):
        return pltpu.make_async_copy(v2_ref.at[:, pl.ds(pl.multiple_of(n * TN, TN), TN)], w2v.at[n], w2s.at[n])

    def start_w13(i, _):
        w13_copy(i, 0).start()
        w13_copy(i, 1).start()
        return 0

    def start_w2(i, _):
        w2_copy(i).start()
        return 0

    lax.fori_loop(0, nf, start_w13, 0)
    lax.fori_loop(0, nn, start_w2, 0)
    barrier(pos)
    tri = strict_upper(t)

    def contrib(s):
        o_copy(s, 0).wait()
        o_copy(s, 1).wait()
        a, _, _ = slots(m_ref[s], pos.me, tri)
        b, _, _ = slots(m_ref[s], pos.mate, tri)
        ab = jnp.concatenate([a, b], axis=0).T.astype(BF16)
        return jnp.dot(ab, ov[s], preferred_element_type=F32)

    def copy(i, n, name):
        return pltpu.make_async_remote_copy(sbuf.at[i], rbuf.at[n], ssem.at[i], rsem.at[n],
                                            device_id=pos.target(name), device_id_type=MESH)

    def got(name):
        copy(0, slot[name], "X").wait_recv()
        return rbuf[slot[name]].astype(F32)

    slot = {name: n for n, name in enumerate(SLOTS)}
    used = []

    def emit(val, name, to):
        i = len(used)
        sbuf[i] = val.astype(BF16)
        c = copy(i, slot[name], to)
        c.start()
        used.append(c)

    for b, to in zip(cut("D3D2D1D0", 2), "XYXY"):
        emit(contrib(rel(b)), "d" + to + b[1], to)

    def column(k):
        for to, other in (("X", "Y"), ("Y", "X")):
            v = contrib(rel(to + k))
            if "d" + other + k in slot:
                v = v + got("d" + other + k)
            emit(v, "c" + to + k, to)

    def share_up(lo, hi):
        def body(i, _):
            w13_copy(i, 0).wait()
            w13_copy(i, 1).wait()
            a = jnp.dot(xv[...], w13[i], preferred_element_type=F32)
            hs[:, pl.ds(pl.multiple_of(i * 128, 128), 128)] = (jax.nn.silu(a[:, :128]) * a[:, 128:]).astype(BF16)
            return 0
        lax.fori_loop(lo, hi, body, 0)

    def share_down():
        def body(n, _):
            w2_copy(n).wait()
            cols = pl.ds(pl.multiple_of(n * TN, TN), TN)
            sh[:, cols] = xv[:, cols].astype(F32) + jnp.dot(hs[...], w2v[n], preferred_element_type=F32)
            return 0
        lax.fori_loop(0, nn, body, 0)

    zs = []

    def along(k):
        v = contrib(rel("C" + k)) + got("cX" + k) + got("cY" + k)
        i = len(used) + len(zs)
        mid_in, mid_to, end_to = cut(HOPS[k], 3)
        link = "Z1" if mid_to[0] == "a" else "Z3"

        @pl.when(pos.mid)
        def _():
            sbuf[i] = (v + got(mid_in)).astype(BF16)
            copy(i, slot[mid_to], link).start()

        @pl.when(jnp.logical_not(pos.mid))
        def _():
            sbuf[i] = v.astype(BF16)
            copy(i, slot[end_to], "Z1").start()
        zs.append(i)

    for k in "3210":
        column(k)
    lx.wait()
    share_up(0, nf)
    along("3")
    share_down()
    along("2")
    along("1")
    v = sh[...] + contrib(rel("C0")) + got("cX0") + got("cY0") + got("az0")
    sh[...] = v

    @pl.when(pos.mid)
    def _():
        y_ref[...] = (sh[...] + got("bz0")).astype(BF16)

    @pl.when(jnp.logical_not(pos.mid))
    def _():
        y_ref[...] = sh[...].astype(BF16)
    for c in used:
        c.wait_send()
    for i in zs:
        copy(i, 0, "X").wait_send()


VLIM = 67043328


def solution(mesh):
    axes = tuple(mesh.axis_names)
    tok = P(axes, None)
    wsp = P(axes, None, None)
    rep = P(None, None)
    ANY = pl.BlockSpec(memory_space=pl.ANY)
    VM = pl.BlockSpec(memory_space=pltpu.VMEM)

    def local(x, ids, gates, w1, w3, w2, ws1, ws3, ws2):
        t, hdim = x.shape
        top = ids.shape[1]
        f = w1.shape[2]
        fs = ws1.shape[1]
        nch = mesh.size // 2
        rows = 8 * CAP
        pad = ((0, 8 - top), (0, 0))
        meta = jnp.concatenate([jnp.pad(ids.T.astype(F32), pad, constant_values=-1.0), jnp.pad(gates.T, pad)], axis=0)
        dma = pltpu.SemaphoreType.DMA
        nsend = 40
        o_same, o_mate, m_same = pl.pallas_call(
            functools.partial(expert_kernel, axes),
            name="experts",
            out_shape=(
                jax.ShapeDtypeStruct((nch, CAP, hdim), BF16),
                jax.ShapeDtypeStruct((nch, CAP, hdim), BF16),
                jax.ShapeDtypeStruct((nch, 16, t), F32),
            ),
            in_specs=[ANY] * 5,
            out_specs=(ANY, ANY, VM),
            scratch_shapes=[
                pltpu.VMEM((2, nch, t, hdim), BF16),
                pltpu.VMEM((2, nch, 16, t), F32),
                pltpu.VMEM((2 * f // 128, hdim, 256), BF16),
                pltpu.VMEM((2 * hdim // TN, f, TN), BF16),
                pltpu.VMEM((rows, hdim), BF16),
                pltpu.VMEM((2, rows, f), BF16),
                pltpu.VMEM((2, rows, 128), F32),
                pltpu.VMEM((2, rows, hdim), BF16),
                dma((nsend,)), dma((2, nch)), dma((nsend,)), dma((2, nch)),
                dma((2,)), dma((2, 2 * f // 128)), dma((2 * hdim // TN,)),
                dma((nch,)), dma((nch,)), dma((nch,)),
            ],
            compiler_params=pltpu.CompilerParams(collective_id=0, has_side_effects=True, vmem_limit_bytes=VLIM),
        )(x, meta, w1, w3, w2)
        y = pl.pallas_call(
            functools.partial(combine_kernel, axes),
            name="combine",
            out_shape=jax.ShapeDtypeStruct((t, hdim), BF16),
            in_specs=[ANY, ANY, VM, ANY, ANY, ANY, ANY],
            out_specs=VM,
            scratch_shapes=[
                pltpu.VMEM((nch, 2 * CAP, hdim), BF16),
                pltpu.VMEM((15, t, hdim), BF16),
                pltpu.VMEM((17, t, hdim), BF16),
                pltpu.VMEM((fs // 128, hdim, 256), BF16),
                pltpu.VMEM((hdim // TN, fs, TN), BF16),
                pltpu.VMEM((t, fs), BF16),
                pltpu.VMEM((t, hdim), F32),
                pltpu.VMEM((t, hdim), BF16),
                dma((2, nch)), dma((15,)), dma((17,)),
                dma((2, fs // 128)), dma((hdim // TN,)), dma((1,)),
            ],
            compiler_params=pltpu.CompilerParams(collective_id=1, has_side_effects=True, vmem_limit_bytes=VLIM),
        )(o_same, o_mate, m_same, x, ws1, ws3, ws2)
        return y

    return jax.shard_map(local, mesh=mesh, in_specs=(tok, tok, tok, wsp, wsp, wsp, rep, rep, rep), out_specs=tok, check_vma=False)
```

```python
import functools

import jax
import jax.numpy as jnp
from jax import lax
from jax.experimental import pallas as pl
from jax.experimental.pallas import tpu as pltpu
from jax.sharding import PartitionSpec as P

CAP = 48
TN = 512
MOST = 4
MESH = pl.DeviceIdType.MESH
F32 = jnp.float32
BF16 = jnp.bfloat16


def cut(text, n):
    return [text[i:i + n] for i in range(0, len(text), n)]


def rel(name):
    return int(name[1]) * 4 + "CXYD".index(name[0])


class Place:
    def __init__(self, axes):
        o, m, i = axes
        self.axes = axes
        self.z = lax.axis_index(o)
        self.y = lax.axis_index(m)
        inner = lax.axis_index(i)
        self.x = inner // 2
        self.c = inner % 2
        self.me = self.z * 8 + self.y * 4 + inner
        self.mate = self.me + 1 - 2 * self.c
        self.chip = {"X": self.me + 2 - 4 * self.x, "Y": self.me + 4 - 8 * self.y}
        self.mid = jnp.logical_and(self.z >= 1, self.z <= 2)
        self.z1 = self.z + 1 - 2 * (self.z % 2)
        self.z3 = 3 - self.z

    def dev(self, z, y, x, c):
        o, m, i = self.axes
        return {o: z, m: y, i: x * 2 + c}

    def target(self, name):
        z, y, x, c = self.z, self.y, self.x, self.c
        return {
            "X": self.dev(z, y, 1 - x, c),
            "Y": self.dev(z, 1 - y, x, c),
            "P": self.dev(z, y, x, 1 - c),
            "Z1": self.dev(self.z1, y, x, c),
            "Z3": self.dev(self.z3, y, x, c),
        }[name]


FLIP = {"X": 1, "Y": 2, "Z1": 4, "Z3": 12, "P": 0}


def barrier(pos):
    sem = pltpu.get_barrier_semaphore()
    for t in ("X", "Y", "P", "Z1"):
        pl.semaphore_signal(sem, inc=1, device_id=pos.target(t), device_id_type=MESH)

    @pl.when(pos.mid)
    def _():
        pl.semaphore_signal(sem, inc=1, device_id=pos.target("Z3"), device_id_type=MESH)
        pl.semaphore_wait(sem, 5)

    @pl.when(jnp.logical_not(pos.mid))
    def _():
        pl.semaphore_wait(sem, 4)


def slots(meta, dev, tri):
    ids = meta[0:8, :]
    gat = meta[8:16, :]
    e0 = (2 * dev).astype(F32)
    m0 = ids == e0
    m1 = ids == e0 + 1.0
    g0 = jnp.sum(jnp.where(m0, gat, 0.0), axis=0, keepdims=True)
    g1 = jnp.sum(jnp.where(m1, gat, 0.0), axis=0, keepdims=True)
    hit = jnp.sum(jnp.where(m0, 1.0, 0.0) + jnp.where(m1, 1.0, 0.0), axis=0, keepdims=True) > 0.5
    hitf = jnp.broadcast_to(jnp.where(hit, 1.0, 0.0), (8, ids.shape[1])).astype(BF16)
    pos = jnp.dot(hitf, tri, preferred_element_type=F32)[0:1, :]
    row = lax.broadcasted_iota(jnp.int32, (CAP, ids.shape[1]), 0).astype(F32)
    oh = jnp.where(jnp.logical_and(row == pos, jnp.where(hit, 1.0, 0.0) > 0.5), 1.0, 0.0)
    return oh, g0, g1


def strict_upper(t):
    a = lax.broadcasted_iota(jnp.int32, (t, t), 0)
    b = lax.broadcasted_iota(jnp.int32, (t, t), 1)
    return jnp.where(a < b, 1.0, 0.0).astype(BF16)


GROUPS = [cut(g, 2) for g in ("C0X0Y0C1", "X1Y1C2", "C3Y2D0", "X2D1X3Y3", "D2D3")]
WHEN = ("1__2", "__3", "__4", "5__6", "__")
EVENTS = {
    1: "C1XC1YC13C31Y0XY0PX0PC1P",
    2: "C2XC2YC21X1YX1PY1PC2P",
    3: "C3XC3YY2XY2PD0PC3P",
    4: "X2PD1P",
    5: "X3YX3PY3P",
    6: "D2PD3P",
}


def expert_kernel(axes, x_ref, m_ref, w1_ref, w3_ref, w2_ref, os_ref, op_ref, mo_ref,
                  xall, mall, w13, w2v, xg, hbuf, gbuf, obuf,
                  xs, xr, ms, mr, ls, ws, w2s, osem, pss, prs):
    pos = Place(axes)
    t, hdim = x_ref.shape
    nf = w1_ref.shape[2] // 128
    nn = hdim // TN
    barrier(pos)
    sends = []

    def send(b, name, own=False):
        dst = rel(b) ^ FLIP[name]
        dc = int(name == "P")
        n = len(sends)

        def make():
            out = []
            for ref, full, ss, rs in ((m_ref, mall, ms, mr), (x_ref, xall, xs, xr)):
                src = ref if own else full.at[0, rel(b)]
                out.append(pltpu.make_async_remote_copy(src, full.at[dc, dst], ss.at[n], rs.at[dc, dst],
                                                        device_id=pos.target(name), device_id_type=MESH))
            return out
        for c in make():
            c.start()
        sends.append(make)

    def arrived(b, dc):
        for ref, full, ss, rs in ((m_ref, mall, ms, mr), (x_ref, xall, xs, xr)):
            pltpu.make_async_remote_copy(ref, full.at[dc, rel(b)], ss.at[0], rs.at[dc, rel(b)],
                                         device_id=pos.target("X"), device_id_type=MESH).wait_recv()

    mid_sends = []

    def mid_send(b, name, own=False):
        pl.when(pos.mid)(lambda: send(b, name, own))
        mid_sends.append(len(sends) - 1)

    for name in ("X", "Y", "Z1"):
        send("C0", name, True)
    mid_send("C0", "Z3", True)
    send("C0", "P", True)
    lx = pltpu.make_async_copy(x_ref, xall.at[0, 0], ls.at[0])
    lm = pltpu.make_async_copy(m_ref, mall.at[0, 0], ls.at[1])
    lx.start()
    lm.start()

    def w13_copy(i, half):
        e, j = i // nf, i % nf
        src = w1_ref if half == 0 else w3_ref
        return pltpu.make_async_copy(src.at[e, :, pl.ds(pl.multiple_of(j * 128, 128), 128)],
                                     w13.at[j, :, pl.ds(pl.multiple_of(e * 256 + half * 128, 128), 128)], ws.at[half, i])

    def w2_copy(i):
        e, n = i // nn, i % nn
        return pltpu.make_async_copy(w2_ref.at[e, :, pl.ds(pl.multiple_of(n * TN, TN), TN)], w2v.at[i], w2s.at[i])

    def start_w13(i, _):
        w13_copy(i, 0).start()
        w13_copy(i, 1).start()
        return 0

    def start_w2(i, _):
        w2_copy(i).start()
        return 0

    lax.fori_loop(0, 2 * nf, start_w13, 0)
    lax.fori_loop(0, 2 * nn, start_w2, 0)

    seen = set()

    def event(n):
        for step in cut(EVENTS[n], 3):
            b, to = step[:2], step[2]
            if b == "C3" and n == 1:
                pl.when(pos.mid)(lambda: arrived(b, 0))
            elif b == "C3" and b not in seen:
                pl.when(jnp.logical_not(pos.mid))(lambda: arrived(b, 0))
                seen.add(b)
            elif b not in seen:
                arrived(b, 0)
                seen.add(b)
            if to in "13":
                mid_send(b, "Z" + to)
            else:
                send(b, to)

    tri = strict_upper(t)
    outs = {}

    def gather_rows(group):
        for b in group:
            arrived(b, 1)
        for dc in range(2):
            for i, b in enumerate(group):
                oh, g0, g1 = slots(mall[dc, rel(b)], pos.me, tri)
                r0 = (dc * len(group) + i) * CAP
                rows = slice(r0, r0 + CAP)
                xg[rows, :] = jnp.dot(oh.astype(BF16), xall[dc, rel(b)], preferred_element_type=F32).astype(BF16)
                for e, g in enumerate((g0, g1)):
                    gbuf[e, rows, :] = jnp.broadcast_to(jnp.sum(oh * g, axis=1, keepdims=True), (CAP, 128))

    def up(m, lo, hi, first):
        def body(j, _):
            if first:
                for e in range(2):
                    w13_copy(e * nf + j, 0).wait()
                    w13_copy(e * nf + j, 1).wait()
            aa = jnp.dot(xg[:m, :], w13[j], preferred_element_type=F32)
            for e in range(2):
                a1 = aa[:, e * 256:e * 256 + 128]
                a3 = aa[:, e * 256 + 128:e * 256 + 256]
                hbuf[e, :m, pl.ds(pl.multiple_of(j * 128, 128), 128)] = (jax.nn.silu(a1) * a3).astype(BF16)
            return 0
        lax.fori_loop(lo, hi, body, 0)

    def down(m, par, first):
        def body(n, _):
            if first:
                w2_copy(n).wait()
                w2_copy(nn + n).wait()
            o0 = jnp.dot(hbuf[0, :m, :], w2v[n], preferred_element_type=F32)
            o1 = jnp.dot(hbuf[1, :m, :], w2v[nn + n], preferred_element_type=F32)
            o = gbuf[0, :m, 0:1] * o0 + gbuf[1, :m, 0:1] * o1
            obuf[par, :m, pl.ds(pl.multiple_of(n * TN, TN), TN)] = o.astype(BF16)
            return 0
        lax.fori_loop(0, nn, body, 0)

    def put(g, par):
        outs[g] = []
        n = len(GROUPS[g])
        for i, b in enumerate(GROUPS[g]):
            s = rel(b)
            a = pltpu.make_async_copy(obuf.at[par, pl.ds(i * CAP, CAP), :], os_ref.at[s], osem.at[s])
            r = pltpu.make_async_remote_copy(obuf.at[par, pl.ds((n + i) * CAP, CAP), :], op_ref.at[s], pss.at[s],
                                             prs.at[s], device_id=pos.target("P"), device_id_type=MESH)
            r.start()
            a.start()
            outs[g].append((a, r))

    def put_done(g):
        for a, r in outs[g]:
            a.wait()
            r.wait_send()

    half = (nf + 1) // 2
    lx.wait()
    lm.wait()
    for g, group in enumerate(GROUPS):
        m = 2 * CAP * len(group)
        before, early, late = WHEN[g].split("_")
        for n in before:
            event(int(n))
        gather_rows(group)
        up(m, 0, half, g == 0)
        for n in early:
            event(int(n))
        up(m, half, nf, g == 0)
        for n in late:
            event(int(n))
        if g >= 2:
            put_done(g - 2)
        down(m, g % 2, g == 0)
        put(g, g % 2)
    last = len(GROUPS)
    mo_ref[...] = mall[0]
    for n, make in enumerate(sends):
        def done(make=make):
            for c in make():
                c.wait_send()
        if n in mid_sends:
            pl.when(pos.mid)(done)
        else:
            done()
    put_done(last - 2)
    put_done(last - 1)
    for g in outs:
        for a, r in outs[g]:
            r.wait_recv()


SLOTS = cut("cX2cX0cY3cY1az0az2az3bz0bz1", 3)
RAW = cut("dX3dX1dY2dY0cX3cX1cY2cY0", 3)
HOPS = {"1": "bz1az0az0", "2": "az2bz1az3", "3": "az3bz0az2"}


def combine_kernel(axes, os_ref, op_ref, m_ref, x_ref, v1_ref, v3_ref, v2_ref, y_ref,
                   ov, sbuf, rbuf, raw, w13, w2v, hs, sh, xv,
                   osem, ssem, rsem, us, ur, ws, w2s, ls):
    pos = Place(axes)
    t, hdim = x_ref.shape
    nf = v1_ref.shape[1] // 128
    nn = hdim // TN
    order = [rel(b) for b in cut("D3D2X3Y3Y2X2D1X1D0C3C2Y1Y0X0C1C0", 2)]

    def o_copy(s, h):
        src = os_ref if h == 0 else op_ref
        return pltpu.make_async_copy(src.at[s], ov.at[s, pl.ds(h * CAP, CAP), :], osem.at[h, s])

    for s in order:
        o_copy(s, 0).start()
        o_copy(s, 1).start()
    lx = pltpu.make_async_copy(x_ref, xv, ls.at[0])
    lx.start()

    def w13_copy(i, half):
        src = v1_ref if half == 0 else v3_ref
        return pltpu.make_async_copy(src.at[:, pl.ds(pl.multiple_of(i * 128, 128), 128)],
                                     w13.at[i, :, pl.ds(half * 128, 128)], ws.at[half, i])

    def w2_copy(n):
        return pltpu.make_async_copy(v2_ref.at[:, pl.ds(pl.multiple_of(n * TN, TN), TN)], w2v.at[n], w2s.at[n])

    def start_w13(i, _):
        w13_copy(i, 0).start()
        w13_copy(i, 1).start()
        return 0

    def start_w2(i, _):
        w2_copy(i).start()
        return 0

    lax.fori_loop(0, nf, start_w13, 0)
    lax.fori_loop(0, nn, start_w2, 0)
    barrier(pos)
    tri = strict_upper(t)

    def spread(s, dev, rows):
        a, _, _ = slots(m_ref[s], dev, tri)
        b, _, _ = slots(m_ref[s], dev + 1 - 2 * pos.c, tri)
        ab = jnp.concatenate([a, b], axis=0).T.astype(BF16)
        return jnp.dot(ab, rows, preferred_element_type=F32)

    loaded = set()

    def load(s):
        if s not in loaded:
            o_copy(s, 0).wait()
            o_copy(s, 1).wait()
            loaded.add(s)

    def contrib(s):
        load(s)
        return spread(s, pos.me, ov[s])

    uslot = {name: n for n, name in enumerate(RAW)}

    def raw_copy(s, n, to):
        return pltpu.make_async_remote_copy(ov.at[s], raw.at[n], us.at[n], ur.at[n],
                                            device_id=pos.target(to), device_id_type=MESH)

    rawsent = []

    def pass_raw(b, to):
        s = rel(b)
        load(s)
        n = uslot[("d" if b[0] == "D" else "c") + to + b[1]]
        c = raw_copy(s, n, to)
        c.start()
        rawsent.append(c)

    def got_raw(name, s):
        n = uslot[name]
        raw_copy(0, n, "X").wait_recv()
        return spread(s, pos.chip[name[1]], raw[n])

    def copy(i, n, name):
        return pltpu.make_async_remote_copy(sbuf.at[i], rbuf.at[n], ssem.at[i], rsem.at[n],
                                            device_id=pos.target(name), device_id_type=MESH)

    def got(name):
        copy(0, slot[name], "X").wait_recv()
        return rbuf[slot[name]].astype(F32)

    slot = {name: n for n, name in enumerate(SLOTS)}
    used = []

    def emit(val, name, to):
        i = len(used)
        sbuf[i] = val.astype(BF16)
        c = copy(i, slot[name], to)
        c.start()
        used.append(c)

    def column(to, k):
        s = rel(to + k)
        other = "X" if to == "Y" else "Y"
        emit(contrib(s) + got_raw("d" + other + k, s), "c" + to + k, to)

    def part(name, s):
        return got(name) if name in slot else got_raw(name, s)

    def share_up(lo, hi):
        def body(i, _):
            w13_copy(i, 0).wait()
            w13_copy(i, 1).wait()
            a = jnp.dot(xv[...], w13[i], preferred_element_type=F32)
            hs[:, pl.ds(pl.multiple_of(i * 128, 128), 128)] = (jax.nn.silu(a[:, :128]) * a[:, 128:]).astype(BF16)
            return 0
        lax.fori_loop(lo, hi, body, 0)

    def share_down():
        def body(n, _):
            w2_copy(n).wait()
            cols = pl.ds(pl.multiple_of(n * TN, TN), TN)
            sh[:, cols] = xv[:, cols].astype(F32) + jnp.dot(hs[...], w2v[n], preferred_element_type=F32)
            return 0
        lax.fori_loop(0, nn, body, 0)

    zs = set()

    def along(k, mid):
        i = 3 + int(k)
        load(rel("C" + k))
        mid_in, mid_to, end_to = cut(HOPS[k], 3)

        @pl.when(pos.mid if mid else jnp.logical_not(pos.mid))
        def _():
            s = rel("C" + k)
            v = spread(s, pos.me, ov[s]) + part("cX" + k, s) + part("cY" + k, s)
            if mid:
                v = v + got(mid_in)
            sbuf[i] = v.astype(BF16)
            name = "Z3" if mid and mid_to[0] == "b" else "Z1"
            copy(i, slot[mid_to if mid else end_to], name).start()
        zs.add(i)

    for b, to in zip(cut("D3D2X3", 2), "XYX"):
        pass_raw(b, to)
    column("Y", "3")
    pass_raw("Y2", "Y")
    column("X", "2")
    for b, to in zip(cut("D1X1D0", 2), "XXY"):
        pass_raw(b, to)
    lx.wait()
    share_up(0, nf // 2)
    along("3", False)
    share_up(nf // 2, nf)
    along("2", False)
    along("2", True)
    column("Y", "1")
    pass_raw("Y0", "Y")
    column("X", "0")
    share_down()
    along("3", True)
    along("1", False)
    along("1", True)
    v = sh[...] + contrib(rel("C0")) + part("cX0", rel("C0")) + part("cY0", rel("C0")) + got("az0")
    sh[...] = v

    @pl.when(pos.mid)
    def _():
        y_ref[...] = (sh[...] + got("bz0")).astype(BF16)

    @pl.when(jnp.logical_not(pos.mid))
    def _():
        y_ref[...] = sh[...].astype(BF16)
    for c in used + rawsent:
        c.wait_send()
    for i in zs:
        copy(i, 0, "X").wait_send()


VLIM = 67043328


def solution(mesh):
    axes = tuple(mesh.axis_names)
    tok = P(axes, None)
    wsp = P(axes, None, None)
    rep = P(None, None)
    ANY = pl.BlockSpec(memory_space=pl.ANY)
    VM = pl.BlockSpec(memory_space=pltpu.VMEM)

    def local(x, ids, gates, w1, w3, w2, ws1, ws3, ws2):
        t, hdim = x.shape
        top = ids.shape[1]
        f = w1.shape[2]
        fs = ws1.shape[1]
        nch = mesh.size // 2
        rows = 2 * MOST * CAP
        pad = ((0, 8 - top), (0, 0))
        meta = jnp.concatenate([jnp.pad(ids.T.astype(F32), pad, constant_values=-1.0), jnp.pad(gates.T, pad)], axis=0)
        dma = pltpu.SemaphoreType.DMA
        nsend = 40
        o_same, o_mate, m_same = pl.pallas_call(
            functools.partial(expert_kernel, axes),
            name="experts",
            out_shape=(
                jax.ShapeDtypeStruct((nch, CAP, hdim), BF16),
                jax.ShapeDtypeStruct((nch, CAP, hdim), BF16),
                jax.ShapeDtypeStruct((nch, 16, t), F32),
            ),
            in_specs=[ANY] * 5,
            out_specs=(ANY, ANY, VM),
            scratch_shapes=[
                pltpu.VMEM((2, nch, t, hdim), BF16),
                pltpu.VMEM((2, nch, 16, t), F32),
                pltpu.VMEM((f // 128, hdim, 512), BF16),
                pltpu.VMEM((2 * hdim // TN, f, TN), BF16),
                pltpu.VMEM((rows, hdim), BF16),
                pltpu.VMEM((2, rows, f), BF16),
                pltpu.VMEM((2, rows, 128), F32),
                pltpu.VMEM((2, rows, hdim), BF16),
                dma((nsend,)), dma((2, nch)), dma((nsend,)), dma((2, nch)),
                dma((2,)), dma((2, 2 * f // 128)), dma((2 * hdim // TN,)),
                dma((nch,)), dma((nch,)), dma((nch,)),
            ],
            compiler_params=pltpu.CompilerParams(collective_id=0, has_side_effects=True, vmem_limit_bytes=VLIM),
        )(x, meta, w1, w3, w2)
        y = pl.pallas_call(
            functools.partial(combine_kernel, axes),
            name="combine",
            out_shape=jax.ShapeDtypeStruct((t, hdim), BF16),
            in_specs=[ANY, ANY, VM, ANY, ANY, ANY, ANY],
            out_specs=VM,
            scratch_shapes=[
                pltpu.VMEM((nch, 2 * CAP, hdim), BF16),
                pltpu.VMEM((7, t, hdim), BF16),
                pltpu.VMEM((len(SLOTS), t, hdim), BF16),
                pltpu.VMEM((len(RAW), 2 * CAP, hdim), BF16),
                pltpu.VMEM((fs // 128, hdim, 256), BF16),
                pltpu.VMEM((hdim // TN, fs, TN), BF16),
                pltpu.VMEM((t, fs), BF16),
                pltpu.VMEM((t, hdim), F32),
                pltpu.VMEM((t, hdim), BF16),
                dma((2, nch)), dma((7,)), dma((len(SLOTS),)), dma((len(RAW),)), dma((len(RAW),)),
                dma((2, fs // 128)), dma((hdim // TN,)), dma((1,)),
            ],
            compiler_params=pltpu.CompilerParams(collective_id=1, has_side_effects=True, vmem_limit_bytes=VLIM),
        )(o_same, o_mate, m_same, x, ws1, ws3, ws2)
        return y

    return jax.shard_map(local, mesh=mesh, in_specs=(tok, tok, tok, wsp, wsp, wsp, rep, rep, rep), out_specs=tok, check_vma=False)
```

```python
import functools

import jax
import jax.numpy as jnp
from jax import lax
from jax.experimental import pallas as pl
from jax.experimental.pallas import tpu as pltpu
from jax.sharding import PartitionSpec as P

CAP = 48
TN = 512
MOST = 4
MESH = pl.DeviceIdType.MESH
F32 = jnp.float32
BF16 = jnp.bfloat16


def cut(text, n):
    return [text[i:i + n] for i in range(0, len(text), n)]


def rel(name):
    return int(name[1]) * 4 + "CXYD".index(name[0])


class Place:
    def __init__(self, axes):
        o, m, i = axes
        self.axes = axes
        self.z = lax.axis_index(o)
        self.y = lax.axis_index(m)
        inner = lax.axis_index(i)
        self.x = inner // 2
        self.c = inner % 2
        self.me = self.z * 8 + self.y * 4 + inner
        self.mate = self.me + 1 - 2 * self.c
        self.chip = {"X": self.me + 2 - 4 * self.x, "Y": self.me + 4 - 8 * self.y}
        self.mid = jnp.logical_and(self.z >= 1, self.z <= 2)
        self.z1 = self.z + 1 - 2 * (self.z % 2)
        self.z3 = 3 - self.z

    def dev(self, z, y, x, c):
        o, m, i = self.axes
        return {o: z, m: y, i: x * 2 + c}

    def target(self, name):
        z, y, x, c = self.z, self.y, self.x, self.c
        return {
            "X": self.dev(z, y, 1 - x, c),
            "Y": self.dev(z, 1 - y, x, c),
            "P": self.dev(z, y, x, 1 - c),
            "Z1": self.dev(self.z1, y, x, c),
            "Z3": self.dev(self.z3, y, x, c),
        }[name]


FLIP = {"X": 1, "Y": 2, "Z1": 4, "Z3": 12, "P": 0}


def barrier(pos):
    sem = pltpu.get_barrier_semaphore()
    for t in ("X", "Y", "P", "Z1"):
        pl.semaphore_signal(sem, inc=1, device_id=pos.target(t), device_id_type=MESH)

    @pl.when(pos.mid)
    def _():
        pl.semaphore_signal(sem, inc=1, device_id=pos.target("Z3"), device_id_type=MESH)
        pl.semaphore_wait(sem, 5)

    @pl.when(jnp.logical_not(pos.mid))
    def _():
        pl.semaphore_wait(sem, 4)


def slots(ids, gat, dev, tri):
    m0 = ids == 2 * dev
    m1 = ids == 2 * dev + 1
    g0 = jnp.sum(jnp.where(m0, gat, 0.0), axis=0, keepdims=True)
    g1 = jnp.sum(jnp.where(m1, gat, 0.0), axis=0, keepdims=True)
    hit = jnp.sum(jnp.where(m0, 1.0, 0.0) + jnp.where(m1, 1.0, 0.0), axis=0, keepdims=True) > 0.5
    hitf = jnp.broadcast_to(jnp.where(hit, 1.0, 0.0), (8, ids.shape[1])).astype(BF16)
    pos = jnp.dot(hitf, tri, preferred_element_type=F32)[0:1, :]
    row = lax.broadcasted_iota(jnp.int32, (CAP, ids.shape[1]), 0).astype(F32)
    oh = jnp.where(jnp.logical_and(row == pos, jnp.where(hit, 1.0, 0.0) > 0.5), 1.0, 0.0)
    return oh, g0, g1


def strict_upper(t):
    a = lax.broadcasted_iota(jnp.int32, (t, t), 0)
    b = lax.broadcasted_iota(jnp.int32, (t, t), 1)
    return jnp.where(a < b, 1.0, 0.0).astype(BF16)


GROUPS = [cut(g, 2) for g in ("C0", "X0Y0C1", "X1Y1C2", "C3Y2D0", "X2D1X3Y3", "D2D3")]
WHEN = ("__1", "__2", "__3", "__4", "5__6", "__")
EVENTS = {
    1: "C1XC1YC13C31Y0XY0PX0PC1P",
    2: "C2XC2YC21X1YX1PY1PC2P",
    3: "C3XC3YY2XY2PD0PC3P",
    4: "X2PD1P",
    5: "X3YX3PY3P",
    6: "D2PD3P",
}


def expert_kernel(axes, x_ref, i_ref, m_ref, w1_ref, w3_ref, w2_ref, os_ref, op_ref, io_ref, mo_ref,
                  xall, iall, mall, w13, w2v, xg, hbuf, gbuf, obuf,
                  xs, xr, js, jr, ms, mr, ls, ws, w2s, osem, pss, prs):
    pos = Place(axes)
    t, hdim = x_ref.shape
    nf = w1_ref.shape[2] // 128
    nn = hdim // TN
    barrier(pos)
    sends = []

    def send(b, name, own=False):
        dst = rel(b) ^ FLIP[name]
        dc = int(name == "P")
        n = len(sends)

        def make():
            out = []
            for ref, full, ss, rs in ((i_ref, iall, js, jr), (m_ref, mall, ms, mr), (x_ref, xall, xs, xr)):
                src = ref if own else full.at[0, rel(b)]
                out.append(pltpu.make_async_remote_copy(src, full.at[dc, dst], ss.at[n], rs.at[dc, dst],
                                                        device_id=pos.target(name), device_id_type=MESH))
            return out
        for c in make():
            c.start()
        sends.append(make)

    def arrived(b, dc):
        for ref, full, ss, rs in ((i_ref, iall, js, jr), (m_ref, mall, ms, mr), (x_ref, xall, xs, xr)):
            pltpu.make_async_remote_copy(ref, full.at[dc, rel(b)], ss.at[0], rs.at[dc, rel(b)],
                                         device_id=pos.target("X"), device_id_type=MESH).wait_recv()

    mid_sends = []

    def mid_send(b, name, own=False):
        pl.when(pos.mid)(lambda: send(b, name, own))
        mid_sends.append(len(sends) - 1)

    for name in ("X", "Y", "Z1"):
        send("C0", name, True)
    mid_send("C0", "Z3", True)
    send("C0", "P", True)
    lx = pltpu.make_async_copy(x_ref, xall.at[0, 0], ls.at[0])
    lm = pltpu.make_async_copy(m_ref, mall.at[0, 0], ls.at[1])
    li = pltpu.make_async_copy(i_ref, iall.at[0, 0], ls.at[2])
    lx.start()
    lm.start()
    li.start()

    def w13_copy(i, half):
        e, j = i // nf, i % nf
        src = w1_ref if half == 0 else w3_ref
        return pltpu.make_async_copy(src.at[e, :, pl.ds(pl.multiple_of(j * 128, 128), 128)],
                                     w13.at[j, :, pl.ds(pl.multiple_of(e * 256 + half * 128, 128), 128)], ws.at[half, i])

    def w2_copy(i):
        e, n = i // nn, i % nn
        return pltpu.make_async_copy(w2_ref.at[e, :, pl.ds(pl.multiple_of(n * TN, TN), TN)], w2v.at[i], w2s.at[i])

    def start_w13(i, _):
        w13_copy(i, 0).start()
        w13_copy(i, 1).start()
        return 0

    def start_w2(i, _):
        w2_copy(i).start()
        return 0

    lax.fori_loop(0, 2 * nf, start_w13, 0)
    lax.fori_loop(0, 2 * nn, start_w2, 0)

    seen = set()

    def event(n):
        for step in cut(EVENTS[n], 3):
            b, to = step[:2], step[2]
            if b == "C3" and n == 1:
                pl.when(pos.mid)(lambda: arrived(b, 0))
            elif b == "C3" and b not in seen:
                pl.when(jnp.logical_not(pos.mid))(lambda: arrived(b, 0))
                seen.add(b)
            elif b not in seen:
                arrived(b, 0)
                seen.add(b)
            if to in "13":
                mid_send(b, "Z" + to)
            else:
                send(b, to)

    tri = strict_upper(t)
    outs = {}

    def gather_rows(group):
        for b in group:
            arrived(b, 1)
        for dc in range(2):
            for i, b in enumerate(group):
                oh, g0, g1 = slots(iall[dc, rel(b)], mall[dc, rel(b)], pos.me, tri)
                r0 = (dc * len(group) + i) * CAP
                rows = slice(r0, r0 + CAP)
                xg[rows, :] = jnp.dot(oh.astype(BF16), xall[dc, rel(b)], preferred_element_type=F32).astype(BF16)
                for e, g in enumerate((g0, g1)):
                    gbuf[e, rows, :] = jnp.broadcast_to(jnp.sum(oh * g, axis=1, keepdims=True), (CAP, 128))

    def up(m, lo, hi, first):
        def body(j, _):
            if first:
                for e in range(2):
                    w13_copy(e * nf + j, 0).wait()
                    w13_copy(e * nf + j, 1).wait()
            aa = jnp.dot(xg[:m, :], w13[j], preferred_element_type=F32)
            for e in range(2):
                a1 = aa[:, e * 256:e * 256 + 128]
                a3 = aa[:, e * 256 + 128:e * 256 + 256]
                hbuf[e, :m, pl.ds(pl.multiple_of(j * 128, 128), 128)] = (jax.nn.silu(a1) * a3).astype(BF16)
            return 0
        lax.fori_loop(lo, hi, body, 0)

    def down(m, par, first):
        def body(n, _):
            if first:
                w2_copy(n).wait()
                w2_copy(nn + n).wait()
            o0 = jnp.dot(hbuf[0, :m, :], w2v[n], preferred_element_type=F32)
            o1 = jnp.dot(hbuf[1, :m, :], w2v[nn + n], preferred_element_type=F32)
            o = gbuf[0, :m, 0:1] * o0 + gbuf[1, :m, 0:1] * o1
            obuf[par, :m, pl.ds(pl.multiple_of(n * TN, TN), TN)] = o.astype(BF16)
            return 0
        lax.fori_loop(0, nn, body, 0)

    def put(g, par):
        outs[g] = []
        n = len(GROUPS[g])
        for i, b in enumerate(GROUPS[g]):
            s = rel(b)
            a = pltpu.make_async_copy(obuf.at[par, pl.ds(i * CAP, CAP), :], os_ref.at[s], osem.at[s])
            r = pltpu.make_async_remote_copy(obuf.at[par, pl.ds((n + i) * CAP, CAP), :], op_ref.at[s], pss.at[s],
                                             prs.at[s], device_id=pos.target("P"), device_id_type=MESH)
            r.start()
            a.start()
            outs[g].append((a, r))

    def put_done(g):
        for a, r in outs[g]:
            a.wait()
            r.wait_send()

    half = (nf + 1) // 2
    lx.wait()
    lm.wait()
    li.wait()
    for g, group in enumerate(GROUPS):
        m = 2 * CAP * len(group)
        before, early, late = WHEN[g].split("_")
        for n in before:
            event(int(n))
        gather_rows(group)
        up(m, 0, half, g == 0)
        for n in early:
            event(int(n))
        up(m, half, nf, g == 0)
        for n in late:
            event(int(n))
        if g >= 2:
            put_done(g - 2)
        down(m, g % 2, g == 0)
        put(g, g % 2)
    last = len(GROUPS)
    io_ref[...] = iall[0]
    mo_ref[...] = mall[0]
    for n, make in enumerate(sends):
        def done(make=make):
            for c in make():
                c.wait_send()
        if n in mid_sends:
            pl.when(pos.mid)(done)
        else:
            done()
    put_done(last - 2)
    put_done(last - 1)
    for g in outs:
        for a, r in outs[g]:
            r.wait_recv()


SLOTS = cut("cX2cX0cY3cY1az0az2az3bz0bz1", 3)
RAW = cut("dX3dX1dY2dY0cX3cX1cY2cY0", 3)
HOPS = {"1": "bz1az0az0", "2": "az2bz1az3", "3": "az3bz0az2"}


def combine_kernel(axes, os_ref, op_ref, i_ref, m_ref, x_ref, v1_ref, v3_ref, v2_ref, y_ref,
                   ov, sbuf, rbuf, raw, w13, w2v, hs, sh, xv,
                   osem, ssem, rsem, us, ur, ws, w2s, ls):
    pos = Place(axes)
    t, hdim = x_ref.shape
    nf = v1_ref.shape[1] // 128
    nn = hdim // TN
    order = [rel(b) for b in cut("D3D2X3Y3Y2X2D1X1D0C3C2Y1Y0X0C1C0", 2)]

    def o_copy(s, h):
        src = os_ref if h == 0 else op_ref
        return pltpu.make_async_copy(src.at[s], ov.at[s, pl.ds(h * CAP, CAP), :], osem.at[h, s])

    for s in order:
        o_copy(s, 0).start()
        o_copy(s, 1).start()
    lx = pltpu.make_async_copy(x_ref, xv, ls.at[0])
    lx.start()

    def w13_copy(i, half):
        src = v1_ref if half == 0 else v3_ref
        return pltpu.make_async_copy(src.at[:, pl.ds(pl.multiple_of(i * 128, 128), 128)],
                                     w13.at[i, :, pl.ds(half * 128, 128)], ws.at[half, i])

    def w2_copy(n):
        return pltpu.make_async_copy(v2_ref.at[:, pl.ds(pl.multiple_of(n * TN, TN), TN)], w2v.at[n], w2s.at[n])

    def start_w13(i, _):
        w13_copy(i, 0).start()
        w13_copy(i, 1).start()
        return 0

    def start_w2(i, _):
        w2_copy(i).start()
        return 0

    lax.fori_loop(0, nf, start_w13, 0)
    lax.fori_loop(0, nn, start_w2, 0)
    barrier(pos)
    tri = strict_upper(t)

    def spread(s, dev, rows):
        a, _, _ = slots(i_ref[s], m_ref[s], dev, tri)
        b, _, _ = slots(i_ref[s], m_ref[s], dev + 1 - 2 * pos.c, tri)
        ab = jnp.concatenate([a, b], axis=0).T.astype(BF16)
        return jnp.dot(ab, rows, preferred_element_type=F32)

    loaded = set()

    def load(s):
        if s not in loaded:
            o_copy(s, 0).wait()
            o_copy(s, 1).wait()
            loaded.add(s)

    def contrib(s):
        load(s)
        return spread(s, pos.me, ov[s])

    uslot = {name: n for n, name in enumerate(RAW)}

    def raw_copy(s, n, to):
        return pltpu.make_async_remote_copy(ov.at[s], raw.at[n], us.at[n], ur.at[n],
                                            device_id=pos.target(to), device_id_type=MESH)

    rawsent = []

    def pass_raw(b, to):
        s = rel(b)
        load(s)
        n = uslot[("d" if b[0] == "D" else "c") + to + b[1]]
        c = raw_copy(s, n, to)
        c.start()
        rawsent.append(c)

    def got_raw(name, s):
        n = uslot[name]
        raw_copy(0, n, "X").wait_recv()
        return spread(s, pos.chip[name[1]], raw[n])

    def copy(i, n, name):
        return pltpu.make_async_remote_copy(sbuf.at[i], rbuf.at[n], ssem.at[i], rsem.at[n],
                                            device_id=pos.target(name), device_id_type=MESH)

    def got(name):
        copy(0, slot[name], "X").wait_recv()
        return rbuf[slot[name]].astype(F32)

    slot = {name: n for n, name in enumerate(SLOTS)}
    used = []

    def emit(val, name, to):
        i = len(used)
        sbuf[i] = val.astype(BF16)
        c = copy(i, slot[name], to)
        c.start()
        used.append(c)

    def column(to, k):
        s = rel(to + k)
        other = "X" if to == "Y" else "Y"
        emit(contrib(s) + got_raw("d" + other + k, s), "c" + to + k, to)

    def part(name, s):
        return got(name) if name in slot else got_raw(name, s)

    def share_up(lo, hi):
        def body(i, _):
            w13_copy(i, 0).wait()
            w13_copy(i, 1).wait()
            a = jnp.dot(xv[...], w13[i], preferred_element_type=F32)
            hs[:, pl.ds(pl.multiple_of(i * 128, 128), 128)] = (jax.nn.silu(a[:, :128]) * a[:, 128:]).astype(BF16)
            return 0
        lax.fori_loop(lo, hi, body, 0)

    def share_down():
        def body(n, _):
            w2_copy(n).wait()
            cols = pl.ds(pl.multiple_of(n * TN, TN), TN)
            sh[:, cols] = xv[:, cols].astype(F32) + jnp.dot(hs[...], w2v[n], preferred_element_type=F32)
            return 0
        lax.fori_loop(0, nn, body, 0)

    zs = set()

    def along(k, mid):
        i = 3 + int(k)
        load(rel("C" + k))
        mid_in, mid_to, end_to = cut(HOPS[k], 3)

        @pl.when(pos.mid if mid else jnp.logical_not(pos.mid))
        def _():
            s = rel("C" + k)
            v = spread(s, pos.me, ov[s]) + part("cX" + k, s) + part("cY" + k, s)
            if mid:
                v = v + got(mid_in)
            sbuf[i] = v.astype(BF16)
            name = "Z3" if mid and mid_to[0] == "b" else "Z1"
            copy(i, slot[mid_to if mid else end_to], name).start()
        zs.add(i)

    for b, to in zip(cut("D3D2X3", 2), "XYX"):
        pass_raw(b, to)
    column("Y", "3")
    pass_raw("Y2", "Y")
    column("X", "2")
    for b, to in zip(cut("D1X1D0", 2), "XXY"):
        pass_raw(b, to)
    lx.wait()
    share_up(0, nf // 2)
    along("3", False)
    share_up(nf // 2, nf)
    along("2", False)
    along("2", True)
    column("Y", "1")
    pass_raw("Y0", "Y")
    column("X", "0")
    share_down()
    along("3", True)
    along("1", False)
    along("1", True)
    v = sh[...] + contrib(rel("C0")) + part("cX0", rel("C0")) + part("cY0", rel("C0")) + got("az0")
    sh[...] = v

    @pl.when(pos.mid)
    def _():
        y_ref[...] = (sh[...] + got("bz0")).astype(BF16)

    @pl.when(jnp.logical_not(pos.mid))
    def _():
        y_ref[...] = sh[...].astype(BF16)
    for c in used + rawsent:
        c.wait_send()
    for i in zs:
        copy(i, 0, "X").wait_send()


VLIM = 67043328


def solution(mesh):
    axes = tuple(mesh.axis_names)
    tok = P(axes, None)
    wsp = P(axes, None, None)
    rep = P(None, None)
    ANY = pl.BlockSpec(memory_space=pl.ANY)
    VM = pl.BlockSpec(memory_space=pltpu.VMEM)

    def local(x, ids, gates, w1, w3, w2, ws1, ws3, ws2):
        t, hdim = x.shape
        top = ids.shape[1]
        f = w1.shape[2]
        fs = ws1.shape[1]
        nch = mesh.size // 2
        rows = 2 * MOST * CAP
        dma = pltpu.SemaphoreType.DMA
        nsend = 40
        o_same, o_mate, i_same, m_same = pl.pallas_call(
            functools.partial(expert_kernel, axes),
            name="experts",
            out_shape=(
                jax.ShapeDtypeStruct((nch, CAP, hdim), BF16),
                jax.ShapeDtypeStruct((nch, CAP, hdim), BF16),
                jax.ShapeDtypeStruct((nch, top, t), jnp.int32),
                jax.ShapeDtypeStruct((nch, top, t), F32),
            ),
            in_specs=[ANY] * 6,
            out_specs=(ANY, ANY, VM, VM),
            scratch_shapes=[
                pltpu.VMEM((2, nch, t, hdim), BF16),
                pltpu.VMEM((2, nch, top, t), jnp.int32),
                pltpu.VMEM((2, nch, top, t), F32),
                pltpu.VMEM((f // 128, hdim, 512), BF16),
                pltpu.VMEM((2 * hdim // TN, f, TN), BF16),
                pltpu.VMEM((rows, hdim), BF16),
                pltpu.VMEM((2, rows, f), BF16),
                pltpu.VMEM((2, rows, 128), F32),
                pltpu.VMEM((2, rows, hdim), BF16),
                dma((nsend,)), dma((2, nch)), dma((nsend,)), dma((2, nch)), dma((nsend,)), dma((2, nch)),
                dma((3,)), dma((2, 2 * f // 128)), dma((2 * hdim // TN,)),
                dma((nch,)), dma((nch,)), dma((nch,)),
            ],
            compiler_params=pltpu.CompilerParams(collective_id=0, has_side_effects=True, vmem_limit_bytes=VLIM),
        )(x, ids.T, gates.T, w1, w3, w2)
        y = pl.pallas_call(
            functools.partial(combine_kernel, axes),
            name="combine",
            out_shape=jax.ShapeDtypeStruct((t, hdim), BF16),
            in_specs=[ANY, ANY, VM, VM, ANY, ANY, ANY, ANY],
            out_specs=VM,
            scratch_shapes=[
                pltpu.VMEM((nch, 2 * CAP, hdim), BF16),
                pltpu.VMEM((7, t, hdim), BF16),
                pltpu.VMEM((len(SLOTS), t, hdim), BF16),
                pltpu.VMEM((len(RAW), 2 * CAP, hdim), BF16),
                pltpu.VMEM((fs // 128, hdim, 256), BF16),
                pltpu.VMEM((hdim // TN, fs, TN), BF16),
                pltpu.VMEM((t, fs), BF16),
                pltpu.VMEM((t, hdim), F32),
                pltpu.VMEM((t, hdim), BF16),
                dma((2, nch)), dma((7,)), dma((len(SLOTS),)), dma((len(RAW),)), dma((len(RAW),)),
                dma((2, fs // 128)), dma((hdim // TN,)), dma((1,)),
            ],
            compiler_params=pltpu.CompilerParams(collective_id=1, has_side_effects=True, vmem_limit_bytes=VLIM),
        )(o_same, o_mate, i_same, m_same, x, ws1, ws3, ws2)
        return y

    return jax.shard_map(local, mesh=mesh, in_specs=(tok, tok, tok, wsp, wsp, wsp, rep, rep, rep), out_specs=tok, check_vma=False)
```
